256 devices in a mesh: ens: 4 (over z_lo, core), gx: 16 (over x, z_hi), gy: 4 (over y).
Axes of the slice: x: 4, y: 4, z: 8 (z_hi: 4, z_lo: 2; z = z_hi * 2 + z_lo), core: 2. Of those that a mesh axis runs over, the one named last changes fastest.
Arguments:
- members: bfloat16 [64, 75, 256, 512], P(('ens', 'gx'), None, None, 'gy'), may hold values from -0.75 to 0.75
- spread: bfloat16 [75, 75], replicated, as said below
- sea_mask: int32 [256, 512], P(('ens', 'gx'), 'gy'), may hold values 0 or 1
- innovations: float32 [75, 256, 512], P(None, ('ens', 'gx'), 'gy'), may hold values from -19 to 19
- obs_error: float32 [75, 256, 512], P(None, ('ens', 'gx'), 'gy'), may hold values from 0.3 to 3
- static_scale: float32 [75, 256, 512], P(None, ('ens', 'gx'), 'gy'), may hold values from 2 to 8
Outputs:
- increment: float32 [75, 256, 512], P(None, ('ens', 'gx'), 'gy')
- alpha_fields: bfloat16 [64, 75, 256, 512], P(('ens', 'gx'), None, None, 'gy')
The draws below stay inside these ranges and needn't reach their ends.
Inputs may be any that keep to these rules, and one draw needn't show every extreme that they name: `spread`: symmetric and positive definite. `sea_mask`: 1 marks sea, 0 land.
All inputs are finite; a program needn't handle non-finite values. No bound on the sum of `sea_mask` on one device may be relied on, other than what follows from the above.
Results may differ from the reference program's by a relative error of at most 0.0065.
Values may be sent and summed in bfloat16 or wider, within the bound.
No kernel may reach another device: no remote copies, remote signals or barrier semaphores. Data moves between devices by JAX's collectives and lax.ppermute only.
A program may use at most 128 MiB of HBM per device.

```python
import math
import jax
import jax.numpy as jnp
from jax import lax

MEMBERS = 64
LAYERS = 75
GRIDS = 3
SWEEPS = 2
COARSE_SWEEPS = 4
ITERATIONS = 3
NX = 256
NY = 512


def draw_spread(key, part):
    noise = jax.random.uniform(key, (LAYERS, LAYERS), jnp.float32, -1.0, 1.0)
    symmetric = 0.45 * (noise + noise.T) / LAYERS
    leading = 1.0 + 0.5 * jax.random.uniform(jax.random.fold_in(key, 7), (LAYERS,), jnp.float32)
    identity = jnp.eye(LAYERS, dtype=jnp.float32)
    return (symmetric * (1.0 - identity) + identity * leading[:, None]).astype(jnp.bfloat16)


def draw_innovations(key, part):
    base = jnp.clip(jax.random.normal(key, (LAYERS, NX, NY), jnp.float32), -4.0, 4.0)
    rising = 3.0 ** (jnp.arange(NX, dtype=jnp.float32) / (NX - 1))
    return 0.5 * base * rising[None, :, None]


def place_ends(drawn, own_key, least, high):
    place = [jax.random.randint(jax.random.fold_in(own_key, axis), (), 0, length) for axis, length in enumerate(drawn.shape)]
    longest = drawn.shape.index(max(drawn.shape))
    neighbour = place[:longest] + [(place[longest] + 1) % drawn.shape[longest]] + place[longest + 1:]
    return drawn.at[tuple(place)].set(least).at[tuple(neighbour)].set(high)


def steps_of(stream_key, shape, cuts, low, top_value):
    factor_of = 1.0
    for axis_at, parts in cuts:
        steps = jax.random.uniform(jax.random.fold_in(jax.random.fold_in(stream_key, 6), axis_at), (parts,), jnp.float32, low / len(cuts), top_value / len(cuts))
        factor_of = factor_of * jnp.repeat(jnp.exp(steps), shape[axis_at] // parts).reshape((-1,) + (1,) * (len(shape) - 1 - axis_at))
    return factor_of


def normal_values(key, extent, deviation, limit, split=(), kind=jnp.bfloat16):
    level = steps_of(key, extent, split, -0.22, 0.18) if split else 1.0
    result = jax.random.normal(key, extent, jnp.float32) * deviation * level
    return jnp.minimum(jnp.maximum(result, -limit), limit).astype(kind)


def setup_inputs(seed: int = 0) -> dict:
    key_list = jax.random.split(jax.random.key(seed), 7)
    return {
        "members": normal_values(key_list[0], (MEMBERS, LAYERS, NX, NY), 0.125, 0.75, ((0, 64), (3, 4))),
        "spread": draw_spread(jax.random.fold_in(key_list[6], 71), 0),
        "sea_mask": place_ends((jax.random.randint(key_list[2], (NX, NY), 0, 8) < 7).astype(jnp.int32), jax.random.fold_in(key_list[2], 1), 0, 1),
        "innovations": draw_innovations(jax.random.fold_in(key_list[6], 71), 0),
        "obs_error": jnp.clip(jnp.exp(math.log(3.0) - 2.3025851 * jax.random.uniform(key_list[4], (LAYERS, NX, NY), jnp.float32) ** steps_of(key_list[4], (LAYERS, NX, NY), ((1, 64), (2, 4)), -0.2, 0.2)), 0.3, 3.0),
        "static_scale": jnp.clip(jnp.exp(math.log(8.0) - 1.3862944 * jax.random.uniform(key_list[5], (LAYERS, NX, NY), jnp.float32) ** steps_of(key_list[5], (LAYERS, NX, NY), ((1, 64), (2, 4)), -0.2, 0.2)), 2.0, 8.0),
    }


diffusivity = 16.0
damping = 0.8


def neighbours(values):
    padded = jnp.pad(values, ((0, 0), (1, 1), (1, 1)))
    return padded[:, 2:, 1:-1] + padded[:, :-2, 1:-1] + padded[:, 1:-1, 2:] + padded[:, 1:-1, :-2]


def apply_level(values, strength):
    return values + strength * (4.0 * values - neighbours(values))


def relax(values, source, strength):
    return values + damping * (source - apply_level(values, strength)) / (1.0 + 4.0 * strength)


def restrict(values):
    layer_count, row_count, column_count = values.shape
    return 0.25 * values.reshape(layer_count, row_count // 2, 2, column_count // 2, 2).sum(axis=(2, 4))


def prolong(values):
    layer_count, row_count, column_count = values.shape
    spread_out = jnp.broadcast_to(values[:, :, None, :, None], (layer_count, row_count, 2, column_count, 2))
    return spread_out.reshape(layer_count, 2 * row_count, 2 * column_count)


def vcycle(source, grid_level):
    strength = diffusivity / 4.0 ** grid_level
    solution = damping / (1.0 + 4.0 * strength) * source
    if grid_level == GRIDS - 1:
        for sweep_index in range(COARSE_SWEEPS - 1):
            solution = relax(solution, source, strength)
        return solution
    for sweep_index in range(SWEEPS - 1):
        solution = relax(solution, source, strength)
    remainder = source - apply_level(solution, strength)
    solution = solution + prolong(vcycle(restrict(remainder), grid_level + 1))
    for sweep_index in range(SWEEPS):
        solution = relax(solution, source, strength)
    return solution


def reference(members, spread, sea_mask, innovations, obs_error, static_scale):
    sea = sea_mask.astype(jnp.float32)[None]

    def member_mix(member, masked):
        product = (member.astype(jnp.float32) * masked).astype(jnp.bfloat16)
        flat = product.reshape(LAYERS, NX * NY)
        return jnp.dot(spread, flat, preferred_element_type=jnp.float32).reshape(LAYERS, NX, NY)

    def covariance(direction):
        masked = sea * direction

        def accumulate(running, member):
            return running + member.astype(jnp.float32) * member_mix(member, masked), None

        ensemble, unused = lax.scan(accumulate, jnp.zeros((LAYERS, NX, NY), jnp.float32), members)
        static = static_scale * vcycle(static_scale * masked, 0)
        return sea * (ensemble + static)

    weights = jnp.zeros((LAYERS, NX, NY), jnp.float32)
    increment = jnp.zeros((LAYERS, NX, NY), jnp.float32)
    residual = innovations
    direction = innovations
    norm_now = jnp.sum(residual * residual)
    for iteration in range(ITERATIONS):
        cov_dir = covariance(direction)
        image = cov_dir + obs_error * direction
        alpha = norm_now / jnp.sum(direction * image)
        weights = weights + alpha * direction
        increment = increment + alpha * cov_dir
        residual = residual - alpha * image
        norm_next = jnp.sum(residual * residual)
        direction = residual + (norm_next / norm_now) * direction
        norm_now = norm_next
    final_mask = sea * weights
    alpha_fields = lax.map(lambda member: member_mix(member, final_mask).astype(jnp.bfloat16), members)
    return increment, alpha_fields
```

```python
import functools

import jax
import jax.numpy as jnp
from jax import lax
from jax.experimental import pallas as pl
from jax.experimental.pallas import tpu as pltpu
from jax.sharding import Mesh
from jax.sharding import PartitionSpec as P

ITERATIONS = 3
DIFFUSIVITY = 16.0
DAMPING = 0.8
ENS_GX = ("ens_0", "ens_1", "gx_0", "gx_1")
ALL = ENS_GX + ("gy",)
LAYERS = 75
PADDED = 76
TILE = 4
FLAT = PADDED * TILE
LANES = 128
STRIDE = 3
F32 = jnp.float32
BF16 = jnp.bfloat16


def swap_halves(first, second):
    upper = lax.broadcasted_iota(jnp.int32, first.shape, 1) < TILE
    return (
        jnp.where(upper, first, pltpu.roll(second, TILE, axis=1)),
        jnp.where(upper, pltpu.roll(first, TILE, axis=1), second),
    )


def to_blocks_kernel(members, out):
    half = PADDED // 2
    for group in range(2):
        rows = members[:, 16 * group : 16 * (group + 1), :].astype(F32)
        for part in range(2):
            chunk = rows[:, 8 * part : 8 * (part + 1), :]
            chunk = jnp.concatenate([chunk, jnp.zeros((1, 8, LANES), F32)], axis=0)
            pairs = chunk.reshape(half, 2, 8, LANES)
            low, high = swap_halves(pairs[:, 0], pairs[:, 1])
            block = 4 * group + 2 * part
            out[block] = low.reshape(FLAT, LANES).astype(BF16)
            out[block + 1] = high.reshape(FLAT, LANES).astype(BF16)


def to_blocks(members):
    layers, rows, lanes = members.shape
    return pl.pallas_call(
        to_blocks_kernel,
        grid=(rows // 32,),
        in_specs=[pl.BlockSpec((layers, 32, lanes), lambda s: (0, s, 0))],
        out_specs=pl.BlockSpec((8, FLAT, lanes), lambda s: (s, 0, 0)),
        out_shape=jax.ShapeDtypeStruct((rows // TILE, FLAT, lanes), BF16),
        name="to_blocks",
    )(members)


def ensemble_kernel(tiles, vector, mixing, out):
    step = pl.program_id(0)
    v = vector[...]
    total = jnp.zeros_like(v)
    for pair in range(tiles.shape[0] // 2):
        first = tiles[2 * pair].astype(F32)
        second = tiles[2 * pair + 1].astype(F32)
        u = jnp.concatenate([(first * v).astype(BF16), (second * v).astype(BF16)], axis=1)
        mixed = jnp.dot(mixing[...], u, preferred_element_type=F32)
        total = total + first * mixed[:, :LANES] + second * mixed[:, LANES:]

    @pl.when(step == 0)
    def _():
        out[...] = total

    @pl.when(step > 0)
    def _():
        out[...] = out[...] + total


def ensemble(tiles, vector, mixing):
    members = tiles.shape[0]
    return pl.pallas_call(
        ensemble_kernel,
        grid=(members // 8,),
        in_specs=[
            pl.BlockSpec((8, FLAT, LANES), lambda s: (s, 0, 0)),
            pl.BlockSpec((FLAT, LANES), lambda s: (0, 0)),
            pl.BlockSpec((FLAT, FLAT), lambda s: (0, 0)),
        ],
        out_specs=pl.BlockSpec((FLAT, LANES), lambda s: (0, 0)),
        out_shape=jax.ShapeDtypeStruct((FLAT, LANES), F32),
        cost_estimate=pl.CostEstimate(
            flops=2 * members * FLAT * FLAT * LANES,
            transcendentals=0,
            bytes_accessed=2 * members * FLAT * LANES,
        ),
        name="ensemble",
    )(tiles, vector, mixing)


def alpha_kernel(members, weights, mixing, out):
    half = PADDED // 2
    for group in range(2):
        parts = []
        for part in range(2):
            block = 4 * group + 2 * part
            u = [
                (
                    members[block + i].astype(F32)
                    * weights[0, (block + i) // 4, 0, (block + i) % 4].astype(F32)
                ).astype(BF16)
                for i in range(2)
            ]
            mixed = jnp.dot(mixing[...], jnp.concatenate(u, axis=1), preferred_element_type=F32)
            low = mixed[:, :LANES].reshape(half, 8, LANES)
            high = mixed[:, LANES:].reshape(half, 8, LANES)
            even, odd = swap_halves(low, high)
            parts.append(jnp.stack([even, odd], axis=1).reshape(PADDED, 8, LANES))
        rows = jnp.concatenate(parts, axis=1).astype(BF16)
        out[:, 16 * group : 16 * (group + 1), :] = rows[:LAYERS]


def alpha(members, weights, mixing):
    blocks = members.shape[0]
    return pl.pallas_call(
        alpha_kernel,
        grid=(blocks // 8,),
        in_specs=[
            pl.BlockSpec((8, FLAT, LANES), lambda s: (s, 0, 0)),
            pl.BlockSpec(
                (1, 2, 1, 4, FLAT, LANES), lambda s: ((s // 2) % 2, s % 2, s // 4, 0, 0, 0)
            ),
            pl.BlockSpec((FLAT, FLAT), lambda s: (0, 0)),
        ],
        out_specs=pl.BlockSpec((LAYERS, 32, LANES), lambda s: (0, s, 0)),
        out_shape=jax.ShapeDtypeStruct((LAYERS, TILE * blocks, LANES), BF16),
        name="alpha",
    )(members, weights, mixing)


def split_dot(left, right, exact_left):
    other = right if exact_left else left
    high = other.astype(BF16)
    low = (other - high.astype(F32)).astype(BF16)
    if exact_left:
        return jnp.dot(left, high, preferred_element_type=F32) + jnp.dot(
            left, low, preferred_element_type=F32
        )
    return jnp.dot(high, right, preferred_element_type=F32) + jnp.dot(
        low, right, preferred_element_type=F32
    )


def around(values):
    rows, columns = values.shape
    row = lax.broadcasted_iota(jnp.int32, values.shape, 0)
    column = lax.broadcasted_iota(jnp.int32, values.shape, 1)
    up = jnp.where(row == 0, 0.0, pltpu.roll(values, 1, axis=0))
    down = jnp.where(row == rows - 1, 0.0, pltpu.roll(values, rows - 1, axis=0))
    left = jnp.where(column == 0, 0.0, pltpu.roll(values, 1, axis=1))
    right = jnp.where(column == columns - 1, 0.0, pltpu.roll(values, columns - 1, axis=1))
    return (up + down) + (left + right)


def pairs_matrix(count, scale, transposed):
    shape = (count, 2 * count) if transposed else (2 * count, count)
    fine = lax.broadcasted_iota(jnp.int32, shape, 1 if transposed else 0)
    coarse = lax.broadcasted_iota(jnp.int32, shape, 0 if transposed else 1)
    return jnp.where(fine // 2 == coarse, scale, 0.0).astype(BF16)


def restrict(values):
    rows, columns = values.shape
    narrow = split_dot(values, pairs_matrix(columns // 2, 0.5, False), False)
    return split_dot(pairs_matrix(rows // 2, 0.5, True), narrow, True)


def prolong(values):
    rows, columns = values.shape
    tall = split_dot(pairs_matrix(rows, 1.0, False), values, True)
    return split_dot(tall, pairs_matrix(columns, 1.0, True), False)


def relax(values, source, strength):
    factor = DAMPING / (1.0 + 4.0 * strength)
    return (1.0 - DAMPING) * values + factor * (source + strength * around(values))


def cycle(source, level):
    strength = DIFFUSIVITY / 4.0**level
    factor = DAMPING / (1.0 + 4.0 * strength)
    values = factor * source
    if level == 2:
        for _ in range(3):
            values = relax(values, source, strength)
        return values
    values = relax(values, source, strength)
    remainder = source - ((1.0 + 4.0 * strength) * values - strength * around(values))
    values = values + prolong(cycle(restrict(remainder), level + 1))
    for _ in range(2):
        values = relax(values, source, strength)
    return values


def cycle_kernel(source, out):
    out[...] = cycle(source[...].astype(F32), 0)


def whole_cycle(source):
    return pl.pallas_call(
        cycle_kernel, out_shape=jax.ShapeDtypeStruct(source.shape, F32), name="cycle"
    )(source)


def flat(values):
    padded = jnp.pad(values, ((0, PADDED - LAYERS), (0, 0), (0, 0)))
    return padded.reshape(FLAT, LANES)


def thirds(value):
    first = lax.reduce_precision(value, 8, 7)
    second = lax.reduce_precision(value - first, 8, 7)
    return [first, second, value - first - second]


def local(members, spread, sea_mask, innovations, obs_error, static_scale):
    place = lax.axis_index(ALL)
    count = lax.axis_size(ALL)
    last = count - 1
    blocks = to_blocks(members.reshape(members.shape[1:]))

    mixing = (
        spread[:, None, :, None] * jnp.eye(TILE, dtype=spread.dtype)[None, :, None, :]
    ).reshape(LAYERS * TILE, LAYERS * TILE)
    mixing = jnp.pad(mixing, ((0, FLAT - LAYERS * TILE),) * 2)
    bound = 36.0 * jnp.max(jnp.sum(jnp.abs(spread.astype(F32)), axis=1)) + 67.0
    shrink = jnp.exp2(-jnp.ceil(jnp.log2(bound)))

    sea = jnp.broadcast_to(sea_mask.astype(F32)[None], (PADDED, TILE, LANES)).reshape(FLAT, LANES)
    scale = sea * flat(static_scale)
    error = shrink * flat(obs_error)
    outer = shrink * sea
    outer_scale = shrink * scale

    def exchange(vector, sums):
        source = (scale * vector).astype(BF16).reshape(PADDED, TILE, LANES)
        send = lax.pad(
            source,
            jnp.zeros((), BF16),
            ((0, count - (STRIDE * (PADDED - 1) + 1), STRIDE - 1), (0, 0, 0), (0, 0, 0)),
        )
        if sums is not None:
            parts = jnp.stack(thirds(sums[0]) + thirds(sums[1])).astype(BF16)
            row = jnp.pad(parts.reshape(1, 1, 6), ((0, 0), (0, TILE - 1), (0, LANES - 6)))
            slot = lax.broadcasted_iota(jnp.int32, (count, 1, 1), 0)
            send = jnp.where(slot == last, row, send)
        got = lax.all_to_all(send, ALL, split_axis=0, concat_axis=0, tiled=True)
        rows = count // 4
        grid = got.reshape(rows, 4, TILE, LANES).transpose(0, 2, 1, 3)
        solved = whole_cycle(grid.reshape(rows * TILE, 4 * LANES))
        back = solved.reshape(rows, TILE, 4, LANES).transpose(0, 2, 1, 3)
        back = back.reshape(count, TILE, LANES)
        if sums is not None:
            total = jnp.sum(got[:, 0, :8].astype(F32), axis=0)
            pair = jnp.stack([total[0] + total[1] + total[2], total[3] + total[4] + total[5]])
            pair = jnp.pad(pair.reshape(1, 1, 2), ((0, 0), (0, TILE - 1), (0, LANES - 2)))
            back = jnp.where(place == last, pair, back)
        result = lax.all_to_all(back, ALL, split_axis=0, concat_axis=0, tiled=True)
        term = result[: STRIDE * PADDED : STRIDE].reshape(FLAT, LANES)
        if sums is None:
            return term, None
        return term, (result[last, 0, 0], result[last, 0, 1])

    tiles = lax.all_to_all(blocks, ENS_GX, split_axis=0, concat_axis=0, tiled=True)

    def image_of(vector, sums):
        term, totals = exchange(vector, sums)
        spread_out = ensemble(tiles, sea * vector, mixing)
        return outer * spread_out + outer_scale * term + error * vector, totals

    def products(residual, along):
        return jnp.sum(residual * residual), jnp.sum(residual * along)

    residual = flat(innovations)
    image, _ = image_of(residual, None)
    weights = increment = direction = along = beyond = None
    norm_before = alpha_before = None
    for iteration in range(ITERATIONS):
        sums = products(residual, image)
        if iteration + 1 < ITERATIONS:
            image_next, (norm, product) = image_of(image, sums)
        else:
            mine = jnp.pad(jnp.stack(sums).reshape(1, 1, 2), ((0, 0), (0, 0), (0, LANES - 2)))
            got = lax.all_to_all(
                jnp.broadcast_to(mine, (count, 1, LANES)),
                ALL,
                split_axis=0,
                concat_axis=0,
                tiled=True,
            )
            norm, product = jnp.sum(got[:, 0, 0]), jnp.sum(got[:, 0, 1])
        if iteration == 0:
            alpha_now = norm / product
            direction, along = residual, image
            weights = alpha_now * direction
            increment = alpha_now * (along - error * direction)
        else:
            ratio = norm / norm_before
            alpha_now = norm / (product - ratio * norm / alpha_before)
            direction = residual + ratio * direction
            along = image + ratio * along
            weights = weights + alpha_now * direction
            increment = increment + alpha_now * (along - error * direction)
        if iteration + 1 < ITERATIONS:
            beyond = image_next if iteration == 0 else image_next + ratio * beyond
            residual = residual - alpha_now * along
            image = image - alpha_now * beyond
        norm_before, alpha_before = norm, alpha_now

    wide = (outer * weights).astype(BF16)[None]
    for axes in ("gx_1", "ens_0", ("ens_1", "gx_0")):
        wide = lax.all_gather(wide, axes, axis=0, tiled=True)
    fields = alpha(blocks, wide.reshape(2, 4, 2, 4, FLAT, LANES), mixing)
    increment = increment.reshape(PADDED, TILE, LANES)[:LAYERS]
    return increment, fields[None]


def solution(mesh):
    split = Mesh(mesh.devices.reshape(2, 2, 4, 4, mesh.shape["gy"]), ALL)
    return jax.shard_map(
        local,
        mesh=split,
        in_specs=(
            P(ENS_GX, None, None, "gy"),
            P(),
            P(ENS_GX, "gy"),
            P(None, ENS_GX, "gy"),
            P(None, ENS_GX, "gy"),
            P(None, ENS_GX, "gy"),
        ),
        out_specs=(P(None, ENS_GX, "gy"), P(ENS_GX, None, None, "gy")),
        check_vma=False,
    )
```

```python
import jax
import jax.numpy as jnp
from jax import lax
from jax.experimental import pallas as pl
from jax.experimental.pallas import tpu as pltpu
from jax.sharding import Mesh
from jax.sharding import PartitionSpec as P


DIFFUSIVITY = 16.0
DAMPING = 0.8
ENS_GX = ("ens_0", "ens_1", "gx_0", "gx_1")
ALL = ENS_GX + ("gy",)
LAYERS = 75
PADDED = 76
TILE = 4
FLAT = PADDED * TILE
LANES = 128
STRIDE = 3
F32 = jnp.float32
BF16 = jnp.bfloat16


def swap_halves(first, second):
    upper = lax.broadcasted_iota(jnp.int32, first.shape, 1) < TILE
    return (
        jnp.where(upper, first, pltpu.roll(second, TILE, axis=1)),
        jnp.where(upper, pltpu.roll(first, TILE, axis=1), second),
    )


def to_blocks_kernel(members, out):
    half = PADDED // 2
    for group in range(2):
        rows = members[:, 16 * group : 16 * (group + 1), :].astype(F32)
        for part in range(2):
            chunk = rows[:, 8 * part : 8 * (part + 1), :]
            chunk = jnp.concatenate([chunk, jnp.zeros((1, 8, LANES), F32)], axis=0)
            pairs = chunk.reshape(half, 2, 8, LANES)
            low, high = swap_halves(pairs[:, 0], pairs[:, 1])
            block = 4 * group + 2 * part
            out[block] = low.reshape(FLAT, LANES).astype(BF16)
            out[block + 1] = high.reshape(FLAT, LANES).astype(BF16)


def to_blocks(members):
    layers, rows, lanes = members.shape
    return pl.pallas_call(
        to_blocks_kernel,
        grid=(rows // 32,),
        in_specs=[pl.BlockSpec((layers, 32, lanes), lambda s: (0, s, 0))],
        out_specs=pl.BlockSpec((8, FLAT, lanes), lambda s: (s, 0, 0)),
        out_shape=jax.ShapeDtypeStruct((rows // TILE, FLAT, lanes), BF16),
        name="to_blocks",
    )(members)


def ensemble_kernel(tiles, vector, mixing, out):
    step = pl.program_id(0)
    v = vector[...]
    total = jnp.zeros_like(v)
    for pair in range(tiles.shape[0] // 2):
        first = tiles[2 * pair].astype(F32)
        second = tiles[2 * pair + 1].astype(F32)
        u = jnp.concatenate([(first * v).astype(BF16), (second * v).astype(BF16)], axis=1)
        mixed = jnp.dot(mixing[...], u, preferred_element_type=F32)
        total = total + first * mixed[:, :LANES] + second * mixed[:, LANES:]

    @pl.when(step == 0)
    def _():
        out[...] = total

    @pl.when(step > 0)
    def _():
        out[...] = out[...] + total


def ensemble(tiles, vector, mixing):
    members = tiles.shape[0]
    return pl.pallas_call(
        ensemble_kernel,
        grid=(members // 8,),
        in_specs=[
            pl.BlockSpec((8, FLAT, LANES), lambda s: (s, 0, 0)),
            pl.BlockSpec((FLAT, LANES), lambda s: (0, 0)),
            pl.BlockSpec((FLAT, FLAT), lambda s: (0, 0)),
        ],
        out_specs=pl.BlockSpec((FLAT, LANES), lambda s: (0, 0)),
        out_shape=jax.ShapeDtypeStruct((FLAT, LANES), F32),
        cost_estimate=pl.CostEstimate(
            flops=2 * members * FLAT * FLAT * LANES,
            transcendentals=0,
            bytes_accessed=2 * members * FLAT * LANES,
        ),
        name="ensemble",
    )(tiles, vector, mixing)


def alpha_kernel(members, weights, mixing, out):
    half = PADDED // 2
    for group in range(2):
        parts = []
        for part in range(2):
            block = 4 * group + 2 * part
            u = [
                (
                    members[block + i].astype(F32)
                    * weights[0, (block + i) // 4, 0, (block + i) % 4].astype(F32)
                ).astype(BF16)
                for i in range(2)
            ]
            mixed = jnp.dot(mixing[...], jnp.concatenate(u, axis=1), preferred_element_type=F32)
            low = mixed[:, :LANES].reshape(half, 8, LANES)
            high = mixed[:, LANES:].reshape(half, 8, LANES)
            even, odd = swap_halves(low, high)
            parts.append(jnp.stack([even, odd], axis=1).reshape(PADDED, 8, LANES))
        rows = jnp.concatenate(parts, axis=1).astype(BF16)
        out[:, 16 * group : 16 * (group + 1), :] = rows[:LAYERS]


def alpha(members, weights, mixing):
    blocks = members.shape[0]
    return pl.pallas_call(
        alpha_kernel,
        grid=(blocks // 8,),
        in_specs=[
            pl.BlockSpec((8, FLAT, LANES), lambda s: (s, 0, 0)),
            pl.BlockSpec(
                (1, 2, 1, 4, FLAT, LANES), lambda s: ((s // 2) % 2, s % 2, s // 4, 0, 0, 0)
            ),
            pl.BlockSpec((FLAT, FLAT), lambda s: (0, 0)),
        ],
        out_specs=pl.BlockSpec((LAYERS, 32, LANES), lambda s: (0, s, 0)),
        out_shape=jax.ShapeDtypeStruct((LAYERS, TILE * blocks, LANES), BF16),
        name="alpha",
    )(members, weights, mixing)


def split_dot(left, right, exact_left):
    other = right if exact_left else left
    high = other.astype(BF16)
    low = (other - high.astype(F32)).astype(BF16)
    if exact_left:
        return jnp.dot(left, high, preferred_element_type=F32) + jnp.dot(
            left, low, preferred_element_type=F32
        )
    return jnp.dot(high, right, preferred_element_type=F32) + jnp.dot(
        low, right, preferred_element_type=F32
    )


def around(values):
    rows, columns = values.shape
    row = lax.broadcasted_iota(jnp.int32, values.shape, 0)
    column = lax.broadcasted_iota(jnp.int32, values.shape, 1)
    up = jnp.where(row == 0, 0.0, pltpu.roll(values, 1, axis=0))
    down = jnp.where(row == rows - 1, 0.0, pltpu.roll(values, rows - 1, axis=0))
    left = jnp.where(column == 0, 0.0, pltpu.roll(values, 1, axis=1))
    right = jnp.where(column == columns - 1, 0.0, pltpu.roll(values, columns - 1, axis=1))
    return (up + down) + (left + right)


def pairs_matrix(count, scale, transposed):
    shape = (count, 2 * count) if transposed else (2 * count, count)
    fine = lax.broadcasted_iota(jnp.int32, shape, 1 if transposed else 0)
    coarse = lax.broadcasted_iota(jnp.int32, shape, 0 if transposed else 1)
    return jnp.where(fine // 2 == coarse, scale, 0.0).astype(BF16)


def restrict(values):
    rows, columns = values.shape
    narrow = split_dot(values, pairs_matrix(columns // 2, 0.5, False), False)
    return split_dot(pairs_matrix(rows // 2, 0.5, True), narrow, True)


def prolong(values):
    rows, columns = values.shape
    tall = split_dot(pairs_matrix(rows, 1.0, False), values, True)
    return split_dot(tall, pairs_matrix(columns, 1.0, True), False)


def relax(values, source, strength):
    factor = DAMPING / (1.0 + 4.0 * strength)
    return (1.0 - DAMPING) * values + factor * (source + strength * around(values))


def cycle(source, level):
    strength = DIFFUSIVITY / 4.0**level
    factor = DAMPING / (1.0 + 4.0 * strength)
    values = factor * source
    if level == 2:
        for _ in range(3):
            values = relax(values, source, strength)
        return values
    values = relax(values, source, strength)
    remainder = source - ((1.0 + 4.0 * strength) * values - strength * around(values))
    values = values + prolong(cycle(restrict(remainder), level + 1))
    for _ in range(2):
        values = relax(values, source, strength)
    return values


def cycle_kernel(place, got, out, grid):
    count = got.shape[0]

    @pl.when(place[0] < count - 2)
    def _():
        for slot in range(count):
            rows, columns = TILE * (slot // 4), LANES * (slot % 4)
            grid[rows : rows + TILE, columns : columns + LANES] = got[slot].astype(F32)
        grid[...] = cycle(grid[...], 0)
        for slot in range(count):
            rows, columns = TILE * (slot // 4), LANES * (slot % 4)
            out[slot] = grid[rows : rows + TILE, columns : columns + LANES]

    @pl.when(place[0] >= count - 2)
    def _():
        lanes = jnp.sum(got[...].astype(F32), axis=0)
        total = jnp.sum(jnp.sum(lanes, axis=0, keepdims=True), axis=1, keepdims=True)
        out[...] = jnp.broadcast_to(total[None], out.shape)


def whole_cycle(place, got):
    count = got.shape[0]
    return pl.pallas_call(
        cycle_kernel,
        in_specs=[
            pl.BlockSpec(memory_space=pltpu.SMEM),
            pl.BlockSpec(memory_space=pltpu.VMEM),
        ],
        out_specs=pl.BlockSpec(memory_space=pltpu.VMEM),
        out_shape=jax.ShapeDtypeStruct(got.shape, F32),
        scratch_shapes=[pltpu.VMEM((count, 4 * LANES), F32)],
        cost_estimate=pl.CostEstimate(
            flops=400 * count * 4 * LANES, transcendentals=0, bytes_accessed=6 * got.size
        ),
        name="cycle",
    )(place, got)


def total_of(values):
    return jnp.sum(jnp.sum(values, axis=0, keepdims=True), axis=1, keepdims=True)


def unpack(result, term):
    for layer in range(PADDED):
        term[TILE * layer : TILE * (layer + 1), :] = result[STRIDE * layer]


def pack(source, residual, image, send, term):
    term[...] = source
    send[...] = jnp.zeros(send.shape, BF16)
    for layer in range(PADDED):
        send[STRIDE * layer] = term[TILE * layer : TILE * (layer + 1), :].astype(BF16)
    for slot, values in ((2, residual * residual), (1, residual * image)):
        left = jnp.sum(values, axis=0, keepdims=True)
        for part in range(3):
            rounded = left.astype(BF16)
            send[send.shape[0] - slot, part : part + 1, :] = rounded
            left = left - rounded.astype(F32)


def applied(result, spread_out, outer, outer_scale, error, vector, term):
    unpack(result, term)
    return outer[...] * spread_out[...] + outer_scale[...] * term[...] + error[...] * vector


def totals(result):
    count = result.shape[0]
    return result[count - 2, 0:1, :], result[count - 1, 0:1, :]


def start_kernel(
    result, spread_out, scale, sea, outer, outer_scale, error, residual, image_out, masked, send, term
):
    r = residual[...]
    w = applied(result, spread_out, outer, outer_scale, error, r, term)
    image_out[...] = w
    masked[...] = sea[...] * w
    pack(scale[...] * w, r, w, send, term)


def first_kernel(
    result,
    spread_out,
    scale,
    sea,
    outer,
    outer_scale,
    error,
    residual,
    image,
    residual_out,
    image_out,
    beyond_out,
    masked,
    send,
    scalars,
    term,
):
    r, w = residual[...], image[...]
    z = applied(result, spread_out, outer, outer_scale, error, w, term)
    norm, product = totals(result)
    step = norm / product
    beyond_out[...] = z
    r_next = r - step * w
    w_next = w - step * z
    residual_out[...] = r_next
    image_out[...] = w_next
    masked[...] = sea[...] * w_next
    scalars[0:1, :] = norm
    scalars[1:2, :] = step
    pack(scale[...] * w_next, r_next, w_next, send, term)


def second_kernel(
    result,
    spread_out,
    outer,
    outer_scale,
    error,
    residual_0,
    image_0,
    beyond_0,
    residual,
    image,
    scalars,
    residual_out,
    direction_out,
    along_out,
    weights_out,
    increment_out,
    image_out,
    send,
    scalars_out,
    term,
):
    r, w = residual[...], image[...]
    n = applied(result, spread_out, outer, outer_scale, error, w, term)
    norm, product = totals(result)
    norm_0, step_0 = scalars[0:1, :], scalars[1:2, :]
    ratio = norm / norm_0
    step = norm / (product - ratio * norm / step_0)
    p = r + ratio * residual_0[...]
    s = w + ratio * image_0[...]
    z = n + ratio * beyond_0[...]
    weights_out[...] = step_0 * residual_0[...] + step * p
    increment_out[...] = step_0 * (image_0[...] - error[...] * residual_0[...]) + step * (
        s - error[...] * p
    )
    r_next = r - step * s
    w_next = w - step * z
    residual_out[...] = r_next
    direction_out[...] = p
    along_out[...] = s
    image_out[...] = w_next
    scalars_out[0:1, :] = norm
    scalars_out[1:2, :] = step
    lane = lax.broadcasted_iota(jnp.int32, (1, LANES), 1)
    both = jnp.where(lane < LANES // 2, total_of(r_next * r_next), total_of(r_next * w_next))
    send[...] = jnp.broadcast_to(both[None], send.shape)


def last_kernel(
    got,
    outer,
    error,
    residual,
    direction,
    along,
    weights,
    increment,
    image,
    scalars,
    wide,
    increment_out,
):
    both = jnp.sum(got[...], axis=0)
    norm, product = both[:, 0:1], both[:, LANES // 2 : LANES // 2 + 1]
    norm_1, step_1 = scalars[0:1, 0:1], scalars[1:2, 0:1]
    ratio = norm / norm_1
    step = norm / (product - ratio * norm / step_1)
    p = residual[...] + ratio * direction[...]
    s = image[...] + ratio * along[...]
    wide[...] = (outer[...] * (weights[...] + step * p)).astype(BF16)
    increment_out[...] = increment[...] + step * (s - error[...] * p)


def kernel_call(body, arguments, outs, scratch=True):
    return pl.pallas_call(
        body,
        in_specs=[pl.BlockSpec(memory_space=pltpu.VMEM)] * len(arguments),
        out_specs=[pl.BlockSpec(memory_space=pltpu.VMEM)] * len(outs),
        out_shape=[jax.ShapeDtypeStruct(shape, kind) for shape, kind in outs],
        scratch_shapes=[pltpu.VMEM((FLAT, LANES), F32)] if scratch else [],
    )(*arguments)


def flat(values):
    padded = jnp.pad(values, ((0, PADDED - LAYERS), (0, 0), (0, 0)))
    return padded.reshape(FLAT, LANES)


def exchanged(values, axes):
    return lax.all_to_all(values, axes, split_axis=0, concat_axis=0, tiled=True)


def window(members, spread, sea_mask, innovations, obs_error, static_scale):
    count = lax.axis_size(ALL)
    place = lax.axis_index(ALL).astype(jnp.int32).reshape(1)
    vector = ((FLAT, LANES), F32)
    packed = ((count, TILE, LANES), BF16)
    blocks = to_blocks(members.reshape(members.shape[1:]))

    sea = jnp.broadcast_to(sea_mask.astype(F32)[None], (PADDED, TILE, LANES)).reshape(FLAT, LANES)
    scale = sea * flat(static_scale)
    residual = flat(innovations)
    source = (scale * residual).astype(BF16).reshape(PADDED, TILE, LANES)
    send = lax.pad(
        source,
        jnp.zeros((), BF16),
        ((0, count - (STRIDE * (PADDED - 1) + 1), STRIDE - 1), (0, 0, 0), (0, 0, 0)),
    )
    got = exchanged(send, ALL)
    tiles = exchanged(blocks, ENS_GX)

    mixing = (
        spread[:, None, :, None] * jnp.eye(TILE, dtype=spread.dtype)[None, :, None, :]
    ).reshape(LAYERS * TILE, LAYERS * TILE)
    mixing = jnp.pad(mixing, ((0, FLAT - LAYERS * TILE),) * 2)
    bound = 36.0 * jnp.max(jnp.sum(jnp.abs(spread.astype(F32)), axis=1)) + 67.0
    shrink = jnp.exp2(-jnp.ceil(jnp.log2(bound)))
    error = shrink * flat(obs_error)
    outer = shrink * sea
    outer_scale = shrink * scale

    def solve(received):
        return exchanged(whole_cycle(place, received), ALL)

    solved = whole_cycle(place, got)
    result = exchanged(solved, ALL)
    spread_out = ensemble(tiles, sea * residual, mixing)
    constants = (outer, outer_scale, error)
    image, masked, send = kernel_call(
        start_kernel,
        (result, spread_out, scale, sea) + constants + (residual,),
        (vector, vector, packed),
    )
    result = solve(exchanged(send, ALL))
    spread_out = ensemble(tiles, masked, mixing)
    residual_1, image_1, beyond, masked, send, scalars = kernel_call(
        first_kernel,
        (result, spread_out, scale, sea) + constants + (residual, image),
        (vector, vector, vector, vector, packed, ((8, LANES), F32)),
    )
    result = solve(exchanged(send, ALL))
    spread_out = ensemble(tiles, masked, mixing)
    residual_2, direction, along, weights, increment, image_2, send, scalars = kernel_call(
        second_kernel,
        (result, spread_out)
        + constants
        + (residual, image, beyond, residual_1, image_1, scalars),
        (vector,) * 6 + (((count, 1, LANES), F32), ((8, LANES), F32)),
    )
    wide, increment = kernel_call(
        last_kernel,
        (
            exchanged(send, ALL),
            outer,
            error,
            residual_2,
            direction,
            along,
            weights,
            increment,
            image_2,
            scalars,
        ),
        (((FLAT, LANES), BF16), vector),
        False,
    )
    wide = wide[None]
    for axes in ("gx_1", "ens_0", ("ens_1", "gx_0")):
        wide = lax.all_gather(wide, axes, axis=0, tiled=True)
    fields = alpha(blocks, wide.reshape(2, 4, 2, 4, FLAT, LANES), mixing)
    increment = increment.reshape(PADDED, TILE, LANES)[:LAYERS]
    return increment, fields[None]


def solution(mesh):
    split = Mesh(mesh.devices.reshape(2, 2, 4, 4, mesh.shape["gy"]), ALL)
    return jax.shard_map(
        window,
        mesh=split,
        in_specs=(
            P(ENS_GX, None, None, "gy"),
            P(),
            P(ENS_GX, "gy"),
            P(None, ENS_GX, "gy"),
            P(None, ENS_GX, "gy"),
            P(None, ENS_GX, "gy"),
        ),
        out_specs=(P(None, ENS_GX, "gy"), P(ENS_GX, None, None, "gy")),
        check_vma=False,
    )
```

```python
import jax
import jax.numpy as jnp
from jax import lax
from jax.experimental import pallas as pl
from jax.experimental.pallas import tpu as pltpu
from jax.sharding import Mesh
from jax.sharding import PartitionSpec as P


DIFFUSIVITY = 16.0
DAMPING = 0.8
ENS_GX = ("ens_0", "ens_1", "gx_0", "gx_1")
ALL = ENS_GX + ("gy",)
LAYERS = 75
PADDED = 76
TILE = 4
FLAT = PADDED * TILE
LANES = 128
STRIDE = 3
F32 = jnp.float32
BF16 = jnp.bfloat16


def swap_halves(first, second):
    upper = lax.broadcasted_iota(jnp.int32, first.shape, 1) < TILE
    return (
        jnp.where(upper, first, pltpu.roll(second, TILE, axis=1)),
        jnp.where(upper, pltpu.roll(first, TILE, axis=1), second),
    )


def to_blocks_kernel(members, out):
    half = PADDED // 2
    for group in range(2):
        rows = members[:, 16 * group : 16 * (group + 1), :].astype(F32)
        for part in range(2):
            chunk = rows[:, 8 * part : 8 * (part + 1), :]
            chunk = jnp.concatenate([chunk, jnp.zeros((1, 8, LANES), F32)], axis=0)
            pairs = chunk.reshape(half, 2, 8, LANES)
            low, high = swap_halves(pairs[:, 0], pairs[:, 1])
            block = 4 * group + 2 * part
            out[block] = low.reshape(FLAT, LANES).astype(BF16)
            out[block + 1] = high.reshape(FLAT, LANES).astype(BF16)


def to_blocks(members):
    layers, rows, lanes = members.shape
    return pl.pallas_call(
        to_blocks_kernel,
        grid=(rows // 32,),
        in_specs=[pl.BlockSpec((layers, 32, lanes), lambda s: (0, s, 0))],
        out_specs=pl.BlockSpec((8, FLAT, lanes), lambda s: (s, 0, 0)),
        out_shape=jax.ShapeDtypeStruct((rows // TILE, FLAT, lanes), BF16),
        name="to_blocks",
    )(members)


def ensemble_kernel(tiles, vector, mixing, out):
    step = pl.program_id(0)
    v = vector[...]
    total = jnp.zeros_like(v)
    for pair in range(tiles.shape[0] // 2):
        first = tiles[2 * pair].astype(F32)
        second = tiles[2 * pair + 1].astype(F32)
        u = jnp.concatenate([(first * v).astype(BF16), (second * v).astype(BF16)], axis=1)
        mixed = jnp.dot(mixing[...], u, preferred_element_type=F32)
        total = total + first * mixed[:, :LANES] + second * mixed[:, LANES:]

    @pl.when(step == 0)
    def _():
        out[...] = total

    @pl.when(step > 0)
    def _():
        out[...] = out[...] + total


def ensemble(tiles, vector, mixing):
    members = tiles.shape[0]
    return pl.pallas_call(
        ensemble_kernel,
        grid=(members // 8,),
        in_specs=[
            pl.BlockSpec((8, FLAT, LANES), lambda s: (s, 0, 0)),
            pl.BlockSpec((FLAT, LANES), lambda s: (0, 0)),
            pl.BlockSpec((FLAT, FLAT), lambda s: (0, 0)),
        ],
        out_specs=pl.BlockSpec((FLAT, LANES), lambda s: (0, 0)),
        out_shape=jax.ShapeDtypeStruct((FLAT, LANES), F32),
        cost_estimate=pl.CostEstimate(
            flops=2 * members * FLAT * FLAT * LANES,
            transcendentals=0,
            bytes_accessed=2 * members * FLAT * LANES,
        ),
        name="ensemble",
    )(tiles, vector, mixing)


def alpha_kernel(members, first, pair, coefficients, mixing, out):
    half = PADDED // 2
    factors = [coefficients[i : i + 1, :] for i in range(3)]

    def weights(x, z):
        return (
            factors[0] * first[0, x, z, 0].astype(F32)
            + factors[1] * pair[0, x, z, 0, 0].astype(F32)
            + factors[2] * pair[0, x, z, 0, 1].astype(F32)
        )

    for group in range(2):
        parts = []
        for part in range(2):
            block = 4 * group + 2 * part
            u = [
                (
                    members[block + i].astype(F32) * weights((block + i) // 4, (block + i) % 4)
                ).astype(BF16)
                for i in range(2)
            ]
            mixed = jnp.dot(mixing[...], jnp.concatenate(u, axis=1), preferred_element_type=F32)
            low = mixed[:, :LANES].reshape(half, 8, LANES)
            high = mixed[:, LANES:].reshape(half, 8, LANES)
            even, odd = swap_halves(low, high)
            parts.append(jnp.stack([even, odd], axis=1).reshape(PADDED, 8, LANES))
        rows = jnp.concatenate(parts, axis=1).astype(BF16)
        out[:, 16 * group : 16 * (group + 1), :] = rows[:LAYERS]


def alpha(members, first, pair, coefficients, mixing):
    blocks = members.shape[0]
    return pl.pallas_call(
        alpha_kernel,
        grid=(blocks // 8,),
        in_specs=[
            pl.BlockSpec((8, FLAT, LANES), lambda s: (s, 0, 0)),
            pl.BlockSpec(
                (1, 2, 4, 1, FLAT, LANES), lambda s: ((s // 2) % 2, s % 2, 0, s // 4, 0, 0)
            ),
            pl.BlockSpec(
                (1, 2, 4, 1, 2, FLAT, LANES), lambda s: ((s // 2) % 2, s % 2, 0, s // 4, 0, 0, 0)
            ),
            pl.BlockSpec((8, LANES), lambda s: (0, 0)),
            pl.BlockSpec((FLAT, FLAT), lambda s: (0, 0)),
        ],
        out_specs=pl.BlockSpec((LAYERS, 32, LANES), lambda s: (0, s, 0)),
        out_shape=jax.ShapeDtypeStruct((LAYERS, TILE * blocks, LANES), BF16),
        name="alpha",
    )(members, first, pair, coefficients, mixing)


def split_dot(left, right, exact_left):
    other = right if exact_left else left
    high = other.astype(BF16)
    low = (other - high.astype(F32)).astype(BF16)
    if exact_left:
        return jnp.dot(left, high, preferred_element_type=F32) + jnp.dot(
            left, low, preferred_element_type=F32
        )
    return jnp.dot(high, right, preferred_element_type=F32) + jnp.dot(
        low, right, preferred_element_type=F32
    )


def around(values):
    rows, columns = values.shape
    row = lax.broadcasted_iota(jnp.int32, values.shape, 0)
    column = lax.broadcasted_iota(jnp.int32, values.shape, 1)
    up = jnp.where(row == 0, 0.0, pltpu.roll(values, 1, axis=0))
    down = jnp.where(row == rows - 1, 0.0, pltpu.roll(values, rows - 1, axis=0))
    left = jnp.where(column == 0, 0.0, pltpu.roll(values, 1, axis=1))
    right = jnp.where(column == columns - 1, 0.0, pltpu.roll(values, columns - 1, axis=1))
    return (up + down) + (left + right)


def pairs_matrix(count, scale, transposed):
    shape = (count, 2 * count) if transposed else (2 * count, count)
    fine = lax.broadcasted_iota(jnp.int32, shape, 1 if transposed else 0)
    coarse = lax.broadcasted_iota(jnp.int32, shape, 0 if transposed else 1)
    return jnp.where(fine // 2 == coarse, scale, 0.0).astype(BF16)


def restrict(values):
    rows, columns = values.shape
    narrow = split_dot(values, pairs_matrix(columns // 2, 0.5, False), False)
    return split_dot(pairs_matrix(rows // 2, 0.5, True), narrow, True)


def prolong(values):
    rows, columns = values.shape
    tall = split_dot(pairs_matrix(rows, 1.0, False), values, True)
    return split_dot(tall, pairs_matrix(columns, 1.0, True), False)


def relax(values, source, strength):
    factor = DAMPING / (1.0 + 4.0 * strength)
    return (1.0 - DAMPING) * values + factor * (source + strength * around(values))


def cycle(source, level):
    strength = DIFFUSIVITY / 4.0**level
    factor = DAMPING / (1.0 + 4.0 * strength)
    values = factor * source
    if level == 2:
        for _ in range(3):
            values = relax(values, source, strength)
        return values
    values = relax(values, source, strength)
    remainder = source - ((1.0 + 4.0 * strength) * values - strength * around(values))
    values = values + prolong(cycle(restrict(remainder), level + 1))
    for _ in range(2):
        values = relax(values, source, strength)
    return values


def cycle_kernel(place, got, out, grid):
    count = got.shape[0]

    @pl.when(place[0] < count - 2)
    def _():
        for slot in range(count):
            rows, columns = TILE * (slot // 4), LANES * (slot % 4)
            grid[rows : rows + TILE, columns : columns + LANES] = got[slot].astype(F32)
        grid[...] = cycle(grid[...], 0)
        for slot in range(count):
            rows, columns = TILE * (slot // 4), LANES * (slot % 4)
            out[slot] = grid[rows : rows + TILE, columns : columns + LANES]

    @pl.when(place[0] >= count - 2)
    def _():
        lanes = jnp.sum(got[...].astype(F32), axis=0)
        total = jnp.sum(jnp.sum(lanes, axis=0, keepdims=True), axis=1, keepdims=True)
        out[...] = jnp.broadcast_to(total[None], out.shape)


def whole_cycle(place, got):
    count = got.shape[0]
    return pl.pallas_call(
        cycle_kernel,
        in_specs=[
            pl.BlockSpec(memory_space=pltpu.SMEM),
            pl.BlockSpec(memory_space=pltpu.VMEM),
        ],
        out_specs=pl.BlockSpec(memory_space=pltpu.VMEM),
        out_shape=jax.ShapeDtypeStruct(got.shape, F32),
        scratch_shapes=[pltpu.VMEM((count, 4 * LANES), F32)],
        cost_estimate=pl.CostEstimate(
            flops=400 * count * 4 * LANES, transcendentals=0, bytes_accessed=6 * got.size
        ),
        name="cycle",
    )(place, got)


def total_of(values):
    return jnp.sum(jnp.sum(values, axis=0, keepdims=True), axis=1, keepdims=True)


def unpack(result, term):
    for layer in range(PADDED):
        term[TILE * layer : TILE * (layer + 1), :] = result[STRIDE * layer]


def pack(source, residual, image, send, term):
    term[...] = source
    send[...] = jnp.zeros(send.shape, BF16)
    for layer in range(PADDED):
        send[STRIDE * layer] = term[TILE * layer : TILE * (layer + 1), :].astype(BF16)
    for slot, values in ((2, residual * residual), (1, residual * image)):
        left = jnp.sum(values, axis=0, keepdims=True)
        for part in range(3):
            rounded = left.astype(BF16)
            send[send.shape[0] - slot, part : part + 1, :] = rounded
            left = left - rounded.astype(F32)


def prepare_kernel(
    innovations, static_scale, sea_mask, residual, scale, sea, masked, halves, send, term
):
    mask = sea_mask[...].astype(F32)
    for layer in range(PADDED):
        rows = slice(TILE * layer, TILE * (layer + 1))
        if layer < LAYERS:
            residual[rows, :] = innovations[layer]
            scale[rows, :] = mask * static_scale[layer]
        else:
            residual[rows, :] = jnp.zeros((TILE, LANES), F32)
            scale[rows, :] = jnp.zeros((TILE, LANES), F32)
        sea[rows, :] = mask
    r = residual[...]
    first = sea[...] * r
    masked[...] = first
    high = first.astype(BF16)
    halves[0] = high
    halves[1] = (first - high.astype(F32)).astype(BF16)
    term[...] = scale[...] * r
    send[...] = jnp.zeros(send.shape, BF16)
    for layer in range(PADDED):
        send[STRIDE * layer] = term[TILE * layer : TILE * (layer + 1), :].astype(BF16)


def constants_kernel(spread, obs_error, scale, sea, mixing, error, outer, outer_scale, shrinks):
    values = spread[...]
    sums = jnp.sum(jnp.abs(values.astype(F32)), axis=1, keepdims=True)
    bound = 36.0 * jnp.max(sums, axis=0, keepdims=True) + 67.0
    shrink = jnp.exp2(-jnp.ceil(jnp.log2(jnp.broadcast_to(bound, (8, LANES)))))
    shrinks[...] = shrink
    row = shrink[0:1, :]
    for layer in range(PADDED):
        rows = slice(TILE * layer, TILE * (layer + 1))
        if layer < LAYERS:
            error[rows, :] = row * obs_error[layer]
        else:
            error[rows, :] = jnp.zeros((TILE, LANES), F32)
    outer[...] = row * sea[...]
    outer_scale[...] = row * scale[...]

    def chooser(shape, long):
        place = lax.broadcasted_iota(jnp.int32, shape, long)
        layer = lax.broadcasted_iota(jnp.int32, shape, 1 - long)
        return jnp.where(place // TILE == layer, 1.0, 0.0).astype(BF16)

    tall = jnp.dot(chooser((FLAT, LAYERS), 0), values, preferred_element_type=F32).astype(BF16)
    full = jnp.dot(tall, chooser((LAYERS, FLAT), 1), preferred_element_type=F32)
    row_in = lax.broadcasted_iota(jnp.int32, full.shape, 0) % TILE
    column_in = lax.broadcasted_iota(jnp.int32, full.shape, 1) % TILE
    mixing[...] = jnp.where(row_in == column_in, full, 0.0).astype(BF16)


def applied(result, spread_out, outer, outer_scale, error, vector, term):
    unpack(result, term)
    return outer[...] * spread_out[...] + outer_scale[...] * term[...] + error[...] * vector


def totals(result):
    count = result.shape[0]
    return result[count - 2, 0:1, :], result[count - 1, 0:1, :]


def start_kernel(
    result,
    spread_out,
    scale,
    sea,
    outer,
    outer_scale,
    error,
    residual,
    image_out,
    masked,
    send,
    term,
):
    r = residual[...]
    w = applied(result, spread_out, outer, outer_scale, error, r, term)
    image_out[...] = w
    masked[...] = sea[...] * w
    pack(scale[...] * w, r, w, send, term)


def first_kernel(
    result,
    spread_out,
    scale,
    sea,
    outer,
    outer_scale,
    error,
    residual,
    image,
    residual_out,
    image_out,
    beyond_out,
    masked,
    pair,
    send,
    scalars,
    term,
):
    r, w = residual[...], image[...]
    z = applied(result, spread_out, outer, outer_scale, error, w, term)
    norm, product = totals(result)
    step = norm / product
    beyond_out[...] = z
    r_next = r - step * w
    w_next = w - step * z
    residual_out[...] = r_next
    image_out[...] = w_next
    masked[...] = sea[...] * w_next
    pair[0] = (sea[...] * r_next).astype(BF16)
    pair[1] = (sea[...] * w_next).astype(BF16)
    scalars[0:1, :] = norm
    scalars[1:2, :] = step
    pack(scale[...] * w_next, r_next, w_next, send, term)


def second_kernel(
    result,
    spread_out,
    outer,
    outer_scale,
    error,
    residual_0,
    image_0,
    beyond_0,
    residual,
    image,
    scalars,
    residual_out,
    direction_out,
    along_out,
    increment_out,
    image_out,
    send,
    scalars_out,
    term,
):
    r, w = residual[...], image[...]
    n = applied(result, spread_out, outer, outer_scale, error, w, term)
    norm, product = totals(result)
    norm_0, step_0 = scalars[0:1, :], scalars[1:2, :]
    ratio = norm / norm_0
    step = norm / (product - ratio * norm / step_0)
    p = r + ratio * residual_0[...]
    s = w + ratio * image_0[...]
    z = n + ratio * beyond_0[...]
    increment_out[...] = step_0 * (image_0[...] - error[...] * residual_0[...]) + step * (
        s - error[...] * p
    )
    r_next = r - step * s
    w_next = w - step * z
    residual_out[...] = r_next
    direction_out[...] = p
    along_out[...] = s
    image_out[...] = w_next
    for i, value in enumerate((norm, step, ratio, step_0)):
        scalars_out[i : i + 1, :] = value
    lane = lax.broadcasted_iota(jnp.int32, (1, LANES), 1)
    both = jnp.where(lane < LANES // 2, total_of(r_next * r_next), total_of(r_next * w_next))
    send[...] = jnp.broadcast_to(both[None], send.shape)


def last_kernel(
    got, error, residual, direction, along, increment, image, scalars, factors, out
):
    both = jnp.sum(got[...], axis=0)
    norm, product = both[:, 0:1], both[:, LANES // 2 : LANES // 2 + 1]
    norm_1, step_1, ratio_1, step_0 = (scalars[i : i + 1, 0:1] for i in range(4))
    ratio = norm / norm_1
    step = norm / (product - ratio * norm / step_1)
    p = residual[...] + ratio * direction[...]
    s = image[...] + ratio * along[...]
    out[...] = increment[...] + step * (s - error[...] * p)
    held = step_1 + step * ratio
    back = step * step_1 * ratio_1 / step_0
    for i, value in enumerate(
        (step_0 + held * ratio_1 - back, held + step + back, -step * step_1)
    ):
        factors[i : i + 1, :] = jnp.broadcast_to(value, (1, LANES))


def kernel_call(body, arguments, outs, scratch=True):
    return pl.pallas_call(
        body,
        in_specs=[pl.BlockSpec(memory_space=pltpu.VMEM)] * len(arguments),
        out_specs=[pl.BlockSpec(memory_space=pltpu.VMEM)] * len(outs),
        out_shape=[jax.ShapeDtypeStruct(shape, kind) for shape, kind in outs],
        scratch_shapes=[pltpu.VMEM((FLAT, LANES), F32)] if scratch else [],
    )(*arguments)


def exchanged(values, axes):
    return lax.all_to_all(values, axes, split_axis=0, concat_axis=0, tiled=True)


def window(members, spread, sea_mask, innovations, obs_error, static_scale):
    count = lax.axis_size(ALL)
    place = lax.axis_index(ALL).astype(jnp.int32).reshape(1)
    vector = ((FLAT, LANES), F32)
    rows = ((8, LANES), F32)
    packed = ((count, TILE, LANES), BF16)
    residual, scale, sea, masked_0, halves, send = kernel_call(
        prepare_kernel,
        (innovations, static_scale, sea_mask),
        (vector,) * 4 + (((2, FLAT, LANES), BF16), packed),
    )
    got = exchanged(send, ALL)
    blocks = to_blocks(members.reshape(members.shape[1:]))
    tiles = exchanged(blocks, ENS_GX)
    mixing, error, outer, outer_scale, shrinks = kernel_call(
        constants_kernel,
        (spread, obs_error, scale, sea),
        (((FLAT, FLAT), BF16),) + (vector,) * 3 + (rows,),
        False,
    )

    def solve(received):
        solved = whole_cycle(place, received)
        return exchanged(solved, ALL)

    def near(values):
        return lax.all_gather(values[None], ("gx_1", "ens_0"), axis=0, tiled=True)

    def far(values):
        got = lax.all_gather(values, ("ens_1", "gx_0"), axis=0, tiled=True)
        return got.reshape((2, 4, 4, 2) + values.shape[1:])

    result = solve(got)
    spread_out = ensemble(tiles, masked_0, mixing)
    constants = (outer, outer_scale, error)
    image, masked, send = kernel_call(
        start_kernel,
        (result, spread_out, scale, sea) + constants + (residual,),
        (vector, vector, packed),
    )
    halves = near(halves)
    opening = halves[:, 0].astype(F32) + halves[:, 1].astype(F32)
    opening = (shrinks[0, 0] * opening).astype(BF16)
    opening = far(opening)
    result = solve(exchanged(send, ALL))
    spread_out = ensemble(tiles, masked, mixing)
    residual_1, image_1, beyond, masked, pair, send, scalars = kernel_call(
        first_kernel,
        (result, spread_out, scale, sea) + constants + (residual, image),
        (vector,) * 4 + (((2, FLAT, LANES), BF16), packed, rows),
    )
    pair = near(pair)
    pair = (shrinks[0, 0] * pair.astype(F32)).astype(BF16)
    pair = far(pair)
    result = solve(exchanged(send, ALL))
    spread_out = ensemble(tiles, masked, mixing)
    residual_2, direction, along, increment, image_2, send, scalars = kernel_call(
        second_kernel,
        (result, spread_out)
        + constants
        + (residual, image, beyond, residual_1, image_1, scalars),
        (vector,) * 5 + (((count, 1, LANES), F32), rows),
    )
    factors, increment = kernel_call(
        last_kernel,
        (
            exchanged(send, ALL),
            error,
            residual_2,
            direction,
            along,
            increment,
            image_2,
            scalars,
        ),
        (rows, vector),
        False,
    )
    fields = alpha(blocks, opening, pair, factors, mixing)
    increment = increment.reshape(PADDED, TILE, LANES)[:LAYERS]
    return increment, fields[None]


def solution(mesh):
    split = Mesh(mesh.devices.reshape(2, 2, 4, 4, mesh.shape["gy"]), ALL)
    return jax.shard_map(
        window,
        mesh=split,
        in_specs=(
            P(ENS_GX, None, None, "gy"),
            P(),
            P(ENS_GX, "gy"),
            P(None, ENS_GX, "gy"),
            P(None, ENS_GX, "gy"),
            P(None, ENS_GX, "gy"),
        ),
        out_specs=(P(None, ENS_GX, "gy"), P(ENS_GX, None, None, "gy")),
        check_vma=False,
    )
```

```python
import jax
import jax.numpy as jnp
from jax import lax
from jax.experimental import pallas as pl
from jax.experimental.pallas import tpu as pltpu
from jax.sharding import Mesh
from jax.sharding import PartitionSpec as P


DIFFUSIVITY = 16.0
DAMPING = 0.8
ENS_GX = ("ens_0", "ens_1", "gx_0", "gx_1")
ALL = ENS_GX + ("gy",)
LAYERS = 75
PADDED = 76
TILE = 4
FLAT = PADDED * TILE
LANES = 128
STRIDE = 3
HALF = TILE // 2
F32 = jnp.float32
BF16 = jnp.bfloat16


def swap_halves(first, second):
    upper = lax.broadcasted_iota(jnp.int32, first.shape, 1) < TILE
    return (
        jnp.where(upper, first, pltpu.roll(second, TILE, axis=1)),
        jnp.where(upper, pltpu.roll(first, TILE, axis=1), second),
    )


def to_blocks_kernel(members, out):
    half = PADDED // 2
    for group in range(2):
        rows = members[:, 16 * group : 16 * (group + 1), :].astype(F32)
        for part in range(2):
            chunk = rows[:, 8 * part : 8 * (part + 1), :]
            chunk = jnp.concatenate([chunk, jnp.zeros((1, 8, LANES), F32)], axis=0)
            pairs = chunk.reshape(half, 2, 8, LANES)
            low, high = swap_halves(pairs[:, 0], pairs[:, 1])
            block = 4 * group + 2 * part
            out[block] = low.reshape(FLAT, LANES).astype(BF16)
            out[block + 1] = high.reshape(FLAT, LANES).astype(BF16)


def to_blocks(members):
    layers, rows, lanes = members.shape
    return pl.pallas_call(
        to_blocks_kernel,
        grid=(rows // 32,),
        in_specs=[pl.BlockSpec((layers, 32, lanes), lambda s: (0, s, 0))],
        out_specs=pl.BlockSpec((8, FLAT, lanes), lambda s: (s, 0, 0)),
        out_shape=jax.ShapeDtypeStruct((rows // TILE, FLAT, lanes), BF16),
        name="to_blocks",
    )(members)


def ensemble_kernel(tiles, vector, mixing, out):
    step = pl.program_id(0)
    v = vector[...]
    total = jnp.zeros_like(v)
    for pair in range(tiles.shape[0] // 2):
        first = tiles[2 * pair].astype(F32)
        second = tiles[2 * pair + 1].astype(F32)
        u = jnp.concatenate([(first * v).astype(BF16), (second * v).astype(BF16)], axis=1)
        mixed = jnp.dot(mixing[...], u, preferred_element_type=F32)
        total = total + first * mixed[:, :LANES] + second * mixed[:, LANES:]

    @pl.when(step == 0)
    def _():
        out[...] = total

    @pl.when(step > 0)
    def _():
        out[...] = out[...] + total


def ensemble(tiles, vector, mixing):
    members = tiles.shape[0]
    return pl.pallas_call(
        ensemble_kernel,
        grid=(members // 8,),
        in_specs=[
            pl.BlockSpec((8, FLAT, LANES), lambda s: (s, 0, 0)),
            pl.BlockSpec((FLAT, LANES), lambda s: (0, 0)),
            pl.BlockSpec((FLAT, FLAT), lambda s: (0, 0)),
        ],
        out_specs=pl.BlockSpec((FLAT, LANES), lambda s: (0, 0)),
        out_shape=jax.ShapeDtypeStruct((FLAT, LANES), F32),
        cost_estimate=pl.CostEstimate(
            flops=2 * members * FLAT * FLAT * LANES,
            transcendentals=0,
            bytes_accessed=2 * members * FLAT * LANES,
        ),
        name="ensemble",
    )(tiles, vector, mixing)


def alpha_kernel(members, first, pair, coefficients, mixing, out):
    half = PADDED // 2
    factors = [coefficients[i : i + 1, :] for i in range(3)]

    def weights(x, z):
        return (
            factors[0] * first[0, x, z, 0].astype(F32)
            + factors[1] * pair[0, x, z, 0, 0].astype(F32)
            + factors[2] * pair[0, x, z, 0, 1].astype(F32)
        )

    for group in range(2):
        parts = []
        for part in range(2):
            block = 4 * group + 2 * part
            u = [
                (
                    members[block + i].astype(F32) * weights((block + i) // 4, (block + i) % 4)
                ).astype(BF16)
                for i in range(2)
            ]
            mixed = jnp.dot(mixing[...], jnp.concatenate(u, axis=1), preferred_element_type=F32)
            low = mixed[:, :LANES].reshape(half, 8, LANES)
            high = mixed[:, LANES:].reshape(half, 8, LANES)
            even, odd = swap_halves(low, high)
            parts.append(jnp.stack([even, odd], axis=1).reshape(PADDED, 8, LANES))
        rows = jnp.concatenate(parts, axis=1).astype(BF16)
        out[:, 16 * group : 16 * (group + 1), :] = rows[:LAYERS]


def alpha(members, first, pair, coefficients, mixing):
    blocks = members.shape[0]
    return pl.pallas_call(
        alpha_kernel,
        grid=(blocks // 8,),
        in_specs=[
            pl.BlockSpec((8, FLAT, LANES), lambda s: (s, 0, 0)),
            pl.BlockSpec(
                (1, 2, 4, 1, FLAT, LANES), lambda s: ((s // 2) % 2, s % 2, 0, s // 4, 0, 0)
            ),
            pl.BlockSpec(
                (1, 2, 4, 1, 2, FLAT, LANES), lambda s: ((s // 2) % 2, s % 2, 0, s // 4, 0, 0, 0)
            ),
            pl.BlockSpec((8, LANES), lambda s: (0, 0)),
            pl.BlockSpec((FLAT, FLAT), lambda s: (0, 0)),
        ],
        out_specs=pl.BlockSpec((LAYERS, 32, LANES), lambda s: (0, s, 0)),
        out_shape=jax.ShapeDtypeStruct((LAYERS, TILE * blocks, LANES), BF16),
        name="alpha",
    )(members, first, pair, coefficients, mixing)


def split_dot(left, right, exact_left):
    other = right if exact_left else left
    high = other.astype(BF16)
    low = (other - high.astype(F32)).astype(BF16)
    if exact_left:
        return jnp.dot(left, high, preferred_element_type=F32) + jnp.dot(
            left, low, preferred_element_type=F32
        )
    return jnp.dot(high, right, preferred_element_type=F32) + jnp.dot(
        low, right, preferred_element_type=F32
    )


def around(values):
    rows, columns = values.shape
    row = lax.broadcasted_iota(jnp.int32, values.shape, 0)
    column = lax.broadcasted_iota(jnp.int32, values.shape, 1)
    up = jnp.where(row == 0, 0.0, pltpu.roll(values, 1, axis=0))
    down = jnp.where(row == rows - 1, 0.0, pltpu.roll(values, rows - 1, axis=0))
    left = jnp.where(column == 0, 0.0, pltpu.roll(values, 1, axis=1))
    right = jnp.where(column == columns - 1, 0.0, pltpu.roll(values, columns - 1, axis=1))
    return (up + down) + (left + right)


def pairs_matrix(count, scale, transposed):
    shape = (count, 2 * count) if transposed else (2 * count, count)
    fine = lax.broadcasted_iota(jnp.int32, shape, 1 if transposed else 0)
    coarse = lax.broadcasted_iota(jnp.int32, shape, 0 if transposed else 1)
    return jnp.where(fine // 2 == coarse, scale, 0.0).astype(BF16)


def restrict(values):
    rows, columns = values.shape
    narrow = split_dot(values, pairs_matrix(columns // 2, 0.5, False), False)
    return split_dot(pairs_matrix(rows // 2, 0.5, True), narrow, True)


def prolong(values):
    rows, columns = values.shape
    tall = split_dot(pairs_matrix(rows, 1.0, False), values, True)
    return split_dot(tall, pairs_matrix(columns, 1.0, True), False)


def relax(values, source, strength):
    factor = DAMPING / (1.0 + 4.0 * strength)
    return (1.0 - DAMPING) * values + factor * (source + strength * around(values))


def cycle(source, level):
    strength = DIFFUSIVITY / 4.0**level
    factor = DAMPING / (1.0 + 4.0 * strength)
    values = factor * source
    if level == 2:
        for _ in range(3):
            values = relax(values, source, strength)
        return values
    values = relax(values, source, strength)
    remainder = source - ((1.0 + 4.0 * strength) * values - strength * around(values))
    values = values + prolong(cycle(restrict(remainder), level + 1))
    for _ in range(2):
        values = relax(values, source, strength)
    return values


def cycle_kernel(place, got, out, grid):
    count = got.shape[0]

    @pl.when(place[0] < count - 2)
    def _():
        for slot in range(count):
            rows, columns = TILE * (slot // 4), LANES * (slot % 4)
            grid[rows : rows + TILE, columns : columns + LANES] = got[slot].astype(F32)
        grid[...] = cycle(grid[...], 0)
        for half in range(2):

            @pl.when((place[0] % STRIDE == 1) == (half == 1))
            def _():
                for slot in range(count):
                    rows, columns = TILE * (slot // 4) + HALF * half, LANES * (slot % 4)
                    out[slot] = grid[rows : rows + HALF, columns : columns + LANES]

    @pl.when(place[0] >= count - 2)
    def _():
        lanes = jnp.sum(got[...].astype(F32), axis=0)
        total = jnp.sum(jnp.sum(lanes, axis=0, keepdims=True), axis=1, keepdims=True)
        out[...] = jnp.broadcast_to(total[None], out.shape)


def whole_cycle(place, got):
    count = got.shape[0]
    return pl.pallas_call(
        cycle_kernel,
        in_specs=[
            pl.BlockSpec(memory_space=pltpu.SMEM),
            pl.BlockSpec(memory_space=pltpu.VMEM),
        ],
        out_specs=pl.BlockSpec(memory_space=pltpu.VMEM),
        out_shape=jax.ShapeDtypeStruct((count, HALF, LANES), F32),
        scratch_shapes=[pltpu.VMEM((count, 4 * LANES), F32)],
        cost_estimate=pl.CostEstimate(
            flops=400 * count * 4 * LANES, transcendentals=0, bytes_accessed=6 * got.size
        ),
        name="cycle",
    )(place, got)


def total_of(values):
    return jnp.sum(jnp.sum(values, axis=0, keepdims=True), axis=1, keepdims=True)


def unpack(result, term):
    for layer in range(PADDED):
        for half in range(2):
            row = TILE * layer + HALF * half
            term[row : row + HALF, :] = result[STRIDE * layer + half]


def pack(source, residual, image, send, term):
    term[...] = source
    send[...] = jnp.zeros(send.shape, BF16)
    for layer in range(PADDED):
        tile = term[TILE * layer : TILE * (layer + 1), :].astype(BF16)
        send[STRIDE * layer] = tile
        send[STRIDE * layer + 1] = tile
    for slot, values in ((2, residual * residual), (1, residual * image)):
        left = jnp.sum(values, axis=0, keepdims=True)
        for part in range(3):
            rounded = left.astype(BF16)
            send[send.shape[0] - slot, part : part + 1, :] = rounded
            left = left - rounded.astype(F32)


def prepare_kernel(
    innovations, static_scale, sea_mask, residual, scale, sea, masked, halves, send, term
):
    mask = sea_mask[...].astype(F32)
    for layer in range(PADDED):
        rows = slice(TILE * layer, TILE * (layer + 1))
        if layer < LAYERS:
            residual[rows, :] = innovations[layer]
            scale[rows, :] = mask * static_scale[layer]
        else:
            residual[rows, :] = jnp.zeros((TILE, LANES), F32)
            scale[rows, :] = jnp.zeros((TILE, LANES), F32)
        sea[rows, :] = mask
    r = residual[...]
    first = sea[...] * r
    masked[...] = first
    high = first.astype(BF16)
    halves[0] = high
    halves[1] = (first - high.astype(F32)).astype(BF16)
    term[...] = scale[...] * r
    send[...] = jnp.zeros(send.shape, BF16)
    for layer in range(PADDED):
        tile = term[TILE * layer : TILE * (layer + 1), :].astype(BF16)
        send[STRIDE * layer] = tile
        send[STRIDE * layer + 1] = tile


def constants_kernel(spread, obs_error, scale, sea, mixing, error, outer, outer_scale, shrinks):
    values = spread[...]
    sums = jnp.sum(jnp.abs(values.astype(F32)), axis=1, keepdims=True)
    bound = 36.0 * jnp.max(sums, axis=0, keepdims=True) + 67.0
    shrink = jnp.exp2(-jnp.ceil(jnp.log2(jnp.broadcast_to(bound, (8, LANES)))))
    shrinks[...] = shrink
    row = shrink[0:1, :]
    for layer in range(PADDED):
        rows = slice(TILE * layer, TILE * (layer + 1))
        if layer < LAYERS:
            error[rows, :] = row * obs_error[layer]
        else:
            error[rows, :] = jnp.zeros((TILE, LANES), F32)
    outer[...] = row * sea[...]
    outer_scale[...] = row * scale[...]

    def chooser(shape, long):
        place = lax.broadcasted_iota(jnp.int32, shape, long)
        layer = lax.broadcasted_iota(jnp.int32, shape, 1 - long)
        return jnp.where(place // TILE == layer, 1.0, 0.0).astype(BF16)

    tall = jnp.dot(chooser((FLAT, LAYERS), 0), values, preferred_element_type=F32).astype(BF16)
    full = jnp.dot(tall, chooser((LAYERS, FLAT), 1), preferred_element_type=F32)
    row_in = lax.broadcasted_iota(jnp.int32, full.shape, 0) % TILE
    column_in = lax.broadcasted_iota(jnp.int32, full.shape, 1) % TILE
    mixing[...] = jnp.where(row_in == column_in, full, 0.0).astype(BF16)


def applied(result, spread_out, outer, outer_scale, error, vector, term):
    unpack(result, term)
    return outer[...] * spread_out[...] + outer_scale[...] * term[...] + error[...] * vector


def totals(result):
    count = result.shape[0]
    return result[count - 2, 0:1, :], result[count - 1, 0:1, :]


def start_kernel(
    result,
    spread_out,
    scale,
    sea,
    outer,
    outer_scale,
    error,
    residual,
    image_out,
    masked,
    send,
    term,
):
    r = residual[...]
    w = applied(result, spread_out, outer, outer_scale, error, r, term)
    image_out[...] = w
    masked[...] = sea[...] * w
    pack(scale[...] * w, r, w, send, term)


def first_kernel(
    result,
    spread_out,
    scale,
    sea,
    outer,
    outer_scale,
    error,
    residual,
    image,
    residual_out,
    image_out,
    beyond_out,
    masked,
    pair,
    send,
    scalars,
    term,
):
    r, w = residual[...], image[...]
    z = applied(result, spread_out, outer, outer_scale, error, w, term)
    norm, product = totals(result)
    step = norm / product
    beyond_out[...] = z
    r_next = r - step * w
    w_next = w - step * z
    residual_out[...] = r_next
    image_out[...] = w_next
    masked[...] = sea[...] * w_next
    pair[0] = (sea[...] * r_next).astype(BF16)
    pair[1] = (sea[...] * w_next).astype(BF16)
    scalars[0:1, :] = norm
    scalars[1:2, :] = step
    pack(scale[...] * w_next, r_next, w_next, send, term)


def second_kernel(
    result,
    spread_out,
    outer,
    outer_scale,
    error,
    residual_0,
    image_0,
    beyond_0,
    residual,
    image,
    scalars,
    residual_out,
    direction_out,
    along_out,
    increment_out,
    image_out,
    send,
    scalars_out,
    term,
):
    r, w = residual[...], image[...]
    n = applied(result, spread_out, outer, outer_scale, error, w, term)
    norm, product = totals(result)
    norm_0, step_0 = scalars[0:1, :], scalars[1:2, :]
    ratio = norm / norm_0
    step = norm / (product - ratio * norm / step_0)
    p = r + ratio * residual_0[...]
    s = w + ratio * image_0[...]
    z = n + ratio * beyond_0[...]
    increment_out[...] = step_0 * (image_0[...] - error[...] * residual_0[...]) + step * (
        s - error[...] * p
    )
    r_next = r - step * s
    w_next = w - step * z
    residual_out[...] = r_next
    direction_out[...] = p
    along_out[...] = s
    image_out[...] = w_next
    for i, value in enumerate((norm, step, ratio, step_0)):
        scalars_out[i : i + 1, :] = value
    lane = lax.broadcasted_iota(jnp.int32, (1, LANES), 1)
    both = jnp.where(lane < LANES // 2, total_of(r_next * r_next), total_of(r_next * w_next))
    send[...] = jnp.broadcast_to(both[None], send.shape)


def last_kernel(
    got, error, residual, direction, along, increment, image, scalars, factors, out
):
    both = jnp.sum(got[...], axis=0)
    norm, product = both[:, 0:1], both[:, LANES // 2 : LANES // 2 + 1]
    norm_1, step_1, ratio_1, step_0 = (scalars[i : i + 1, 0:1] for i in range(4))
    ratio = norm / norm_1
    step = norm / (product - ratio * norm / step_1)
    p = residual[...] + ratio * direction[...]
    s = image[...] + ratio * along[...]
    out[...] = increment[...] + step * (s - error[...] * p)
    held = step_1 + step * ratio
    back = step * step_1 * ratio_1 / step_0
    for i, value in enumerate(
        (step_0 + held * ratio_1 - back, held + step + back, -step * step_1)
    ):
        factors[i : i + 1, :] = jnp.broadcast_to(value, (1, LANES))


def kernel_call(body, arguments, outs, scratch=True):
    return pl.pallas_call(
        body,
        in_specs=[pl.BlockSpec(memory_space=pltpu.VMEM)] * len(arguments),
        out_specs=[pl.BlockSpec(memory_space=pltpu.VMEM)] * len(outs),
        out_shape=[jax.ShapeDtypeStruct(shape, kind) for shape, kind in outs],
        scratch_shapes=[pltpu.VMEM((FLAT, LANES), F32)] if scratch else [],
    )(*arguments)


def exchanged(values, axes):
    return lax.all_to_all(values, axes, split_axis=0, concat_axis=0, tiled=True)


def window(members, spread, sea_mask, innovations, obs_error, static_scale):
    count = lax.axis_size(ALL)
    place = lax.axis_index(ALL).astype(jnp.int32).reshape(1)
    vector = ((FLAT, LANES), F32)
    rows = ((8, LANES), F32)
    packed = ((count, TILE, LANES), BF16)
    residual, scale, sea, masked_0, halves, send = kernel_call(
        prepare_kernel,
        (innovations, static_scale, sea_mask),
        (vector,) * 4 + (((2, FLAT, LANES), BF16), packed),
    )
    got = exchanged(send, ALL)
    blocks = to_blocks(members.reshape(members.shape[1:]))
    tiles = exchanged(blocks, ENS_GX)
    mixing, error, outer, outer_scale, shrinks = kernel_call(
        constants_kernel,
        (spread, obs_error, scale, sea),
        (((FLAT, FLAT), BF16),) + (vector,) * 3 + (rows,),
        False,
    )

    def solve(received):
        solved = whole_cycle(place, received)
        return exchanged(solved, ALL)

    def near(values):
        return lax.all_gather(values[None], ("gx_1", "ens_0"), axis=0, tiled=True)

    def far(values):
        got = lax.all_gather(values, ("ens_1", "gx_0"), axis=0, tiled=True)
        return got.reshape((2, 4, 4, 2) + values.shape[1:])

    result = solve(got)
    spread_out = ensemble(tiles, masked_0, mixing)
    constants = (outer, outer_scale, error)
    image, masked, send = kernel_call(
        start_kernel,
        (result, spread_out, scale, sea) + constants + (residual,),
        (vector, vector, packed),
    )
    halves = near(halves)
    opening = halves[:, 0].astype(F32) + halves[:, 1].astype(F32)
    opening = (shrinks[0, 0] * opening).astype(BF16)
    opening = far(opening)
    result = solve(exchanged(send, ALL))
    spread_out = ensemble(tiles, masked, mixing)
    residual_1, image_1, beyond, masked, pair, send, scalars = kernel_call(
        first_kernel,
        (result, spread_out, scale, sea) + constants + (residual, image),
        (vector,) * 4 + (((2, FLAT, LANES), BF16), packed, rows),
    )
    pair = near(pair)
    pair = (shrinks[0, 0] * pair.astype(F32)).astype(BF16)
    pair = far(pair)
    result = solve(exchanged(send, ALL))
    spread_out = ensemble(tiles, masked, mixing)
    residual_2, direction, along, increment, image_2, send, scalars = kernel_call(
        second_kernel,
        (result, spread_out)
        + constants
        + (residual, image, beyond, residual_1, image_1, scalars),
        (vector,) * 5 + (((count, 1, LANES), F32), rows),
    )
    factors, increment = kernel_call(
        last_kernel,
        (
            exchanged(send, ALL),
            error,
            residual_2,
            direction,
            along,
            increment,
            image_2,
            scalars,
        ),
        (rows, vector),
        False,
    )
    fields = alpha(blocks, opening, pair, factors, mixing)
    increment = increment.reshape(PADDED, TILE, LANES)[:LAYERS]
    return increment, fields[None]


def solution(mesh):
    split = Mesh(mesh.devices.reshape(2, 2, 4, 4, mesh.shape["gy"]), ALL)
    return jax.shard_map(
        window,
        mesh=split,
        in_specs=(
            P(ENS_GX, None, None, "gy"),
            P(),
            P(ENS_GX, "gy"),
            P(None, ENS_GX, "gy"),
            P(None, ENS_GX, "gy"),
            P(None, ENS_GX, "gy"),
        ),
        out_specs=(P(None, ENS_GX, "gy"), P(ENS_GX, None, None, "gy")),
        check_vma=False,
    )
```
